32 devices in a mesh: role: 4 (over z), tp: 4 (over y, x), dp: 2 (over core).
Axes of the slice: x: 2, y: 2, z: 4, core: 2. Of those that a mesh axis runs over, the one named last changes fastest.
Arguments:
- master: float32 [1024, 8192], P('tp', ('role', 'dp')), may hold values from -0.0625 to 0.0625
- key_bias: float32 [1024], P('tp'), may hold values from -3 to 3
- probe_tokens: bfloat16 [2048, 8192], P(('role', 'dp')), may hold values from -6 to 6
Outputs:
- weight: bfloat16 [8192, 1024], P(None, 'tp')
- probe_keys: bfloat16 [2048, 1024], P(('role', 'dp'), 'tp')
- checksum: float32 [8192], replicated
The draws below stay inside these ranges and needn't reach their ends.
All inputs are finite; a program needn't handle non-finite values.
Results may differ from the reference program's by a relative error of at most 0.005.
Values may be sent and summed in bfloat16 or wider, within the bound.
A program may use at most 64 MiB of HBM per device.

```python
import jax
import jax.numpy as jnp

D = 8192
KVW = 1024
PROBES = 2048


def level_of(own_key, shape, cuts, least, largest):
    factor_of, own = 1.0, jax.random.fold_in(own_key, 6)
    for dim, parts in cuts:
        draws = jnp.exp(jax.random.uniform(jax.random.fold_in(own, dim), (parts,), jnp.float32, least / len(cuts), largest / len(cuts)))
        factor_of = factor_of * jnp.repeat(draws, shape[dim] // parts).reshape([-1 if axis == dim else 1 for axis in range(len(shape))])
    return factor_of


def bell_draw(stream_key, extent, scale, bound, pieces=(), kind=jnp.bfloat16):
    level = level_of(stream_key, extent, pieces, -0.22, 0.18) if pieces else 1.0
    values = jax.random.normal(stream_key, extent, jnp.float32) * scale * level
    return jnp.minimum(jnp.maximum(values, -bound), bound).astype(kind)


def setup_inputs(seed: int = 0) -> dict:
    keys = jax.random.split(jax.random.key(seed), 4)
    return {
        "master": bell_draw(keys[0], (KVW, D), D ** -0.5, 0.0625, ((0, 4), (1, 8)), jnp.float32),
        "key_bias": bell_draw(keys[1], (KVW,), 0.5, 3.0, ((0, 4),), jnp.float32),
        "probe_tokens": bell_draw(keys[2], (PROBES, D), 1.0, 6.0, ((0, 8),)),
    }


def reference(master, key_bias, probe_tokens):
    weight = jnp.transpose(master).astype(jnp.bfloat16)
    projected = jnp.dot(probe_tokens, weight, preferred_element_type=jnp.float32)
    probe_keys = (projected + key_bias[None, :]).astype(jnp.bfloat16)
    checksum = jnp.sum(weight.astype(jnp.float32), axis=1)
    return weight, probe_keys, checksum
```

```python
import functools

import jax
import jax.numpy as jnp
from jax import lax
from jax.experimental import pallas as pl
from jax.experimental.pallas import tpu as pltpu
from jax.sharding import PartitionSpec as P

MESH = pl.DeviceIdType.MESH


def gather_kernel(
    n, reps, heads, rows, chunk,
    master, bias, probe, full, keys, sums,
    slab, tokens, acc, part, got,
    slab_sem, token_sem, send_sem, line_sem, pass_sem, peer_sem,
    part_send, part_recv, sum_send, sum_recv, sum_pass, sum_peer,
):
    pieces = rows // chunk
    me, rep, head = lax.axis_index("role"), lax.axis_index("dp"), lax.axis_index("tp")
    has_left, has_right = me > 0, me < n - 1
    bits = [1 << s for s in range(heads.bit_length() - 1)]

    def pair(bit):
        return head + bit * (1 - 2 * lax.rem(lax.div(head, bit), 2))

    def peer_of(p):
        return lax.rem(rep + 1 + p, reps)

    barrier = pltpu.get_barrier_semaphore()

    @pl.when(has_left)
    def _():
        pl.semaphore_signal(barrier, inc=1, device_id={"role": me - 1}, device_id_type=MESH)

    @pl.when(has_right)
    def _():
        pl.semaphore_signal(barrier, inc=1, device_id={"role": me + 1}, device_id_type=MESH)

    @pl.loop(0, reps - 1)
    def _(p):
        pl.semaphore_signal(barrier, inc=1, device_id={"dp": peer_of(p)}, device_id_type=MESH)

    for bit in bits:
        pl.semaphore_signal(barrier, inc=1, device_id={"tp": pair(bit)}, device_id_type=MESH)

    def slab_copy(k):
        return pltpu.make_async_copy(
            master.at[:, pl.ds(k * chunk, chunk)], slab.at[k], slab_sem.at[k]
        )

    token_copy = pltpu.make_async_copy(probe, tokens, token_sem)
    for k in range(pieces):
        slab_copy(k).start()
    token_copy.start()

    def at(r, d, k):
        start = (r * reps + d) * rows + k * chunk
        return full.at[pl.ds(pl.multiple_of(start, chunk), chunk)]

    def line(r, k, way):
        return pltpu.make_async_remote_copy(
            src_ref=at(r, rep, k), dst_ref=at(r, rep, k),
            send_sem=send_sem.at[way, r, k], recv_sem=line_sem.at[r, k],
            device_id={"role": me + 2 * way - 1}, device_id_type=MESH,
        )

    def share(r, k, p):
        return pltpu.make_async_remote_copy(
            src_ref=at(r, rep, k), dst_ref=at(r, rep, k),
            send_sem=pass_sem.at[p, r, k], recv_sem=peer_sem.at[rep, r, k],
            device_id={"dp": peer_of(p)}, device_id_type=MESH,
        )

    def wait_line(r, k):
        pltpu.make_async_copy(at(r, rep, k), at(r, rep, k), line_sem.at[r, k]).wait()

    def wait_peer(r, d, k):
        pltpu.make_async_copy(at(r, d, k), at(r, d, k), peer_sem.at[d, r, k]).wait()

    def sum_line(r, way):
        b = r * reps + rep
        return pltpu.make_async_remote_copy(
            src_ref=sums.at[b], dst_ref=sums.at[b],
            send_sem=sum_send.at[way, r], recv_sem=sum_recv.at[r],
            device_id={"role": me + 2 * way - 1}, device_id_type=MESH,
        )

    def sum_share(r, p):
        b = r * reps + rep
        return pltpu.make_async_remote_copy(
            src_ref=sums.at[b], dst_ref=sums.at[b],
            send_sem=sum_pass.at[p, r], recv_sem=sum_peer.at[rep, r],
            device_id={"dp": peer_of(p)}, device_id_type=MESH,
        )

    def send_own(k):
        @pl.when(has_left)
        def _():
            line(me, k, 0).start()

        @pl.when(has_right)
        def _():
            line(me, k, 1).start()

        @pl.loop(0, reps - 1)
        def _(p):
            share(me, k, p).start()

    for k in range(pieces):
        slab_copy(k).wait()
        block = slab[k].astype(jnp.bfloat16).astype(jnp.float32)
        at(me, rep, k)[...] = jnp.transpose(block).astype(jnp.bfloat16)
        part[0, k : k + 1, :] = jnp.sum(block, axis=0, keepdims=True)
        if k == 0:
            beside = jnp.where(has_left & has_right, 2, 1) if n > 2 else n - 1
            pl.semaphore_wait(barrier, reps - 1 + len(bits) + beside)
        else:
            send_own(k - 1)
    acc[...] = jnp.broadcast_to(bias[...], acc.shape)
    send_own(pieces - 1)

    def trade(s):
        return pltpu.make_async_remote_copy(
            src_ref=part.at[s], dst_ref=got.at[s],
            send_sem=part_send.at[s], recv_sem=part_recv.at[s],
            device_id={"tp": pair(bits[s])}, device_id_type=MESH,
        )

    early = chunk % 128 == 0

    def add_dot(r, d, k):
        if early:
            start = (r * reps + d) * rows + k * chunk
            cols = pl.ds(pl.multiple_of(start, chunk), chunk)
            acc[...] += jnp.dot(
                tokens[:, cols], at(r, d, k)[...], preferred_element_type=jnp.float32
            )

    def peers_done(r, k):
        @pl.loop(0, reps - 1)
        def _(p):
            d = peer_of(p)
            wait_peer(r, d, k)
            add_dot(r, d, k)

    trade(0).start()
    token_copy.wait()

    @pl.loop(0, pieces)
    def _(k):
        add_dot(me, rep, k)

    for s in range(len(bits)):
        trade(s).wait_recv()
        total = part[s] + got[s]
        if s + 1 < len(bits):
            part[s + 1] = total
        else:
            sums[me * reps + rep] = total
        half = (pieces * s // len(bits), pieces * (s + 1) // len(bits))

        @pl.loop(half[0], half[1])
        def _(k):
            peers_done(me, k)

        if s + 1 < len(bits):
            trade(s + 1).start()

    @pl.when(has_left)
    def _():
        sum_line(me, 0).start()

    @pl.when(has_right)
    def _():
        sum_line(me, 1).start()

    @pl.loop(0, reps - 1)
    def _(p):
        sum_share(me, p).start()

    def sides(h):
        low, high = me - h, me + h
        return (
            (low, low >= 0, has_right, 1),
            (high, high < n, has_left, 0),
        )

    def step(t, fresh, lagged):
        if fresh:
            h, k = 1 + lax.div(t, pieces), lax.rem(t, pieces)
            for r, here, onward, way in sides(h):
                @pl.when(here)
                def _():
                    wait_line(r, k)

                    @pl.when(onward)
                    def _():
                        line(r, k, way).start()

                    @pl.loop(0, reps - 1)
                    def _(p):
                        share(r, k, p).start()

                    @pl.when(k == pieces - 1)
                    def _():
                        b = r * reps + rep
                        pltpu.make_async_copy(sums.at[b], sums.at[b], sum_recv.at[r]).wait()

                        @pl.when(onward)
                        def _():
                            sum_line(r, way).start()

                        @pl.loop(0, reps - 1)
                        def _(p):
                            sum_share(r, p).start()

            for r, here, onward, way in sides(h):
                @pl.when(here)
                def _():
                    add_dot(r, rep, k)

        if lagged:
            h, k = 1 + lax.div(t - 1, pieces), lax.rem(t - 1, pieces)
            for r, here, onward, way in sides(h):
                @pl.when(here)
                def _():
                    peers_done(r, k)

    steps = (n - 1) * pieces
    step(jnp.int32(0), True, False)

    @pl.loop(1, steps)
    def _(t):
        step(t, True, True)

    step(jnp.int32(steps), False, True)

    @pl.loop(0, n)
    def _(r):
        @pl.loop(0, reps - 1)
        def _(p):
            b = r * reps + peer_of(p)
            pltpu.make_async_copy(sums.at[b], sums.at[b], sum_peer.at[peer_of(p), r]).wait()
            sum_share(r, p).wait_send()

        for onward, way in (((r >= me) & has_left, 0), ((r <= me) & has_right, 1)):
            @pl.when(onward)
            def _():
                sum_line(r, way).wait_send()

        @pl.loop(0, pieces)
        def _(k):
            @pl.loop(0, reps - 1)
            def _(p):
                share(r, k, p).wait_send()

            for onward, way in (((r >= me) & has_left, 0), ((r <= me) & has_right, 1)):
                @pl.when(onward)
                def _():
                    line(r, k, way).wait_send()

    for s in range(len(bits)):
        trade(s).wait_send()

    if not early:
        tile = 512

        @pl.loop(0, tokens.shape[1] // tile)
        def _(i):
            span = pl.ds(pl.multiple_of(i * tile, tile), tile)
            acc[...] += jnp.dot(
                tokens[:, span], full[span, :], preferred_element_type=jnp.float32
            )

    keys[...] = acc[...].astype(keys.dtype)


def store_kernel(full, keys, sums, weight, probe_keys, checksum, sems):
    parts = 8
    size = full.shape[0] // parts
    copies = [
        pltpu.make_async_copy(
            full.at[pl.ds(i * size, size)], weight.at[pl.ds(i * size, size)], sems.at[i]
        )
        for i in range(parts)
    ]
    copies.append(pltpu.make_async_copy(keys, probe_keys, sems.at[parts]))
    copies.append(pltpu.make_async_copy(sums, checksum, sems.at[parts + 1]))
    for copy in copies:
        copy.start()
    for copy in copies:
        copy.wait()


def body(mesh, master, key_bias, probe_tokens):
    n, reps, heads = mesh.shape["role"], mesh.shape["dp"], mesh.shape["tp"]
    feats, rows = master.shape
    probes, width = probe_tokens.shape
    chunk = min(128, rows)
    pieces, blocks = rows // chunk, n * reps
    levels = heads.bit_length() - 1
    vmem, hbm = pl.BlockSpec(memory_space=pltpu.VMEM), pl.BlockSpec(memory_space=pl.ANY)
    dma = pltpu.SemaphoreType.DMA
    others = max(reps - 1, 1)
    full, keys, sums = pl.pallas_call(
        functools.partial(gather_kernel, n, reps, heads, rows, chunk),
        out_shape=(
            pltpu.VMEM((width, feats), jnp.bfloat16),
            pltpu.VMEM((probes, feats), jnp.bfloat16),
            pltpu.VMEM((blocks, pieces, chunk), jnp.float32),
        ),
        in_specs=[hbm, vmem, hbm],
        out_specs=(vmem, vmem, vmem),
        scratch_shapes=[
            pltpu.VMEM((pieces, feats, chunk), jnp.float32),
            pltpu.VMEM((probes, width), jnp.bfloat16),
            pltpu.VMEM((probes, feats), jnp.float32),
            pltpu.VMEM((levels, pieces, chunk), jnp.float32),
            pltpu.VMEM((levels, pieces, chunk), jnp.float32),
            dma((pieces,)),
            dma,
            dma((2, n, pieces)),
            dma((n, pieces)),
            dma((others, n, pieces)),
            dma((reps, n, pieces)),
            dma((levels,)),
            dma((levels,)),
            dma((2, n)),
            dma((n,)),
            dma((others, n)),
            dma((reps, n)),
        ],
        compiler_params=pltpu.CompilerParams(
            collective_id=0, has_side_effects=True, vmem_limit_bytes=24 * 2**20
        ),
        name="gather",
    )(
        pltpu.with_memory_space_constraint(master, pltpu.HBM),
        key_bias.reshape(1, feats),
        pltpu.with_memory_space_constraint(probe_tokens, pltpu.HBM),
    )
    weight, probe_keys, checksum = pl.pallas_call(
        store_kernel,
        out_shape=(
            jax.ShapeDtypeStruct(full.shape, full.dtype),
            jax.ShapeDtypeStruct(keys.shape, keys.dtype),
            jax.ShapeDtypeStruct(sums.shape, sums.dtype),
        ),
        in_specs=[vmem] * 3,
        out_specs=(hbm,) * 3,
        scratch_shapes=[dma((10,))],
        compiler_params=pltpu.CompilerParams(vmem_limit_bytes=2**20),
        name="store",
    )(*(pltpu.with_memory_space_constraint(x, pltpu.VMEM) for x in (full, keys, sums)))
    return weight, probe_keys, checksum.reshape(-1)


def solution(mesh):
    placed = (P("tp", ("role", "dp")), P("tp"), P(("role", "dp"), None))
    return jax.shard_map(
        functools.partial(body, mesh),
        mesh=mesh,
        in_specs=placed,
        out_specs=(P(None, "tp"), P(("role", "dp"), "tp"), P()),
        check_vma=False,
    )
```

```python
import functools

import jax
import jax.numpy as jnp
from jax import lax
from jax.experimental import pallas as pl
from jax.experimental.pallas import tpu as pltpu
from jax.sharding import PartitionSpec as P

MESH = pl.DeviceIdType.MESH


def gather_kernel(
    n, reps, heads, rows, chunk,
    master, bias, probe, full, keys, sums,
    slab, tokens, offset, acc, part, got,
    slab_sem, token_sem, bias_sem, send_sem, line_sem, pass_sem, peer_sem,
    part_send, part_recv, sum_send, sum_recv, sum_pass, sum_peer,
):
    pieces = rows // chunk
    me, rep, head = lax.axis_index("role"), lax.axis_index("dp"), lax.axis_index("tp")
    has_left, has_right = me > 0, me < n - 1
    bits = [1 << s for s in range(heads.bit_length() - 1)]

    def pair(bit):
        return head + bit * (1 - 2 * lax.rem(lax.div(head, bit), 2))

    def peer_of(p):
        return lax.rem(rep + 1 + p, reps)

    barrier = pltpu.get_barrier_semaphore()

    @pl.when(has_left)
    def _():
        pl.semaphore_signal(barrier, inc=1, device_id={"role": me - 1}, device_id_type=MESH)

    @pl.when(has_right)
    def _():
        pl.semaphore_signal(barrier, inc=1, device_id={"role": me + 1}, device_id_type=MESH)

    @pl.loop(0, reps - 1)
    def _(p):
        pl.semaphore_signal(barrier, inc=1, device_id={"dp": peer_of(p)}, device_id_type=MESH)

    for bit in bits:
        pl.semaphore_signal(barrier, inc=1, device_id={"tp": pair(bit)}, device_id_type=MESH)

    def slab_copy(i):
        cols = pl.ds(0, chunk) if i == 0 else pl.ds(chunk, rows - chunk)
        return pltpu.make_async_copy(master.at[:, cols], slab.at[:, cols], slab_sem.at[i])

    slabs = min(pieces, 2)
    token_copy = pltpu.make_async_copy(probe, tokens, token_sem)
    bias_copy = pltpu.make_async_copy(bias, offset, bias_sem)
    for i in range(slabs):
        slab_copy(i).start()
    bias_copy.start()
    token_copy.start()

    def block(r, d):
        return full.at[pl.ds(pl.multiple_of((r * reps + d) * rows, chunk), rows)]

    def slot(r, owner):
        return lax.rem(r - owner + 2 * n - 1, n)

    def at(r, d, k):
        start = (r * reps + d) * rows + k * chunk
        return full.at[pl.ds(pl.multiple_of(start, chunk), chunk)]

    def line(r, k, way):
        return pltpu.make_async_remote_copy(
            src_ref=at(r, rep, k), dst_ref=at(r, rep, k),
            send_sem=send_sem.at[way, r],
            recv_sem=line_sem.at[slot(r, me + 2 * way - 1), k],
            device_id={"role": me + 2 * way - 1}, device_id_type=MESH,
        )

    def share(r, k, p):
        return pltpu.make_async_remote_copy(
            src_ref=at(r, rep, k), dst_ref=at(r, rep, k),
            send_sem=pass_sem.at[p, r], recv_sem=peer_sem.at[reps - 2 - p, r, k],
            device_id={"dp": peer_of(p)}, device_id_type=MESH,
        )

    def wait_line(r, k):
        pltpu.make_async_copy(at(r, rep, k), at(r, rep, k), line_sem.at[slot(r, me), k]).wait()

    def wait_peer(r, p, k):
        here = at(r, peer_of(p), k)
        pltpu.make_async_copy(here, here, peer_sem.at[p, r, k]).wait()

    def sum_line(r, way):
        b = r * reps + rep
        return pltpu.make_async_remote_copy(
            src_ref=sums.at[b], dst_ref=sums.at[b],
            send_sem=sum_send.at[way, r],
            recv_sem=sum_recv.at[slot(r, me + 2 * way - 1)],
            device_id={"role": me + 2 * way - 1}, device_id_type=MESH,
        )

    def sum_share(r, p):
        b = r * reps + rep
        return pltpu.make_async_remote_copy(
            src_ref=sums.at[b], dst_ref=sums.at[b],
            send_sem=sum_pass.at[p, r], recv_sem=sum_peer.at[reps - 2 - p, r],
            device_id={"dp": peer_of(p)}, device_id_type=MESH,
        )

    def send_own(k):
        @pl.when(has_left)
        def _():
            line(me, k, 0).start()

        @pl.when(has_right)
        def _():
            line(me, k, 1).start()

        @pl.loop(0, reps - 1)
        def _(p):
            share(me, k, p).start()

    for k in range(pieces):
        if k < 2:
            slab_copy(k).wait()
        held = slab[:, k * chunk : (k + 1) * chunk].astype(jnp.bfloat16).astype(jnp.float32)
        at(me, rep, k)[...] = jnp.transpose(held).astype(jnp.bfloat16)
        part[0, k : k + 1, :] = jnp.sum(held, axis=0, keepdims=True)
        if k == min(1, pieces - 1):
            beside = jnp.where(has_left & has_right, 2, 1) if n > 2 else n - 1
            pl.semaphore_wait(barrier, reps - 1 + len(bits) + beside)
        if k:
            send_own(k - 1)
    bias_copy.wait()
    acc[...] = jnp.broadcast_to(offset[...], acc.shape)
    send_own(pieces - 1)

    def trade(s):
        return pltpu.make_async_remote_copy(
            src_ref=part.at[s], dst_ref=got.at[s],
            send_sem=part_send.at[s], recv_sem=part_recv.at[s],
            device_id={"tp": pair(bits[s])}, device_id_type=MESH,
        )

    early = chunk % 128 == 0

    def add_dot(r, d, k):
        if early:
            start = (r * reps + d) * rows + k * chunk
            cols = pl.ds(pl.multiple_of(start, chunk), chunk)
            acc[...] += jnp.dot(
                tokens[:, cols], at(r, d, k)[...], preferred_element_type=jnp.float32
            )

    def peers_done(r, k):
        @pl.loop(0, reps - 1)
        def _(p):
            wait_peer(r, p, k)
            add_dot(r, peer_of(p), k)

    trade(0).start()
    token_copy.wait()

    @pl.loop(0, pieces)
    def _(k):
        add_dot(me, rep, k)

    for s in range(len(bits)):
        trade(s).wait_recv()
        total = part[s] + got[s]
        if s + 1 < len(bits):
            part[s + 1] = total
        else:
            sums[me * reps + rep] = total
        half = (pieces * s // len(bits), pieces * (s + 1) // len(bits))

        @pl.loop(half[0], half[1])
        def _(k):
            peers_done(me, k)

        if s + 1 < len(bits):
            trade(s + 1).start()

    @pl.when(has_left)
    def _():
        sum_line(me, 0).start()

    @pl.when(has_right)
    def _():
        sum_line(me, 1).start()

    @pl.loop(0, reps - 1)
    def _(p):
        sum_share(me, p).start()

    def sides(h):
        low, high = me - h, me + h
        return (
            (low, low >= 0, has_right, 1),
            (high, high < n, has_left, 0),
        )

    def step(t, fresh, lagged):
        if fresh:
            h, k = 1 + lax.div(t, pieces), lax.rem(t, pieces)
            for r, here, onward, way in sides(h):
                @pl.when(here)
                def _():
                    wait_line(r, k)

                    @pl.when(onward)
                    def _():
                        line(r, k, way).start()

                    @pl.loop(0, reps - 1)
                    def _(p):
                        share(r, k, p).start()

                    @pl.when(k == pieces - 1)
                    def _():
                        b = r * reps + rep
                        pltpu.make_async_copy(sums.at[b], sums.at[b], sum_recv.at[slot(r, me)]).wait()

                        @pl.when(onward)
                        def _():
                            sum_line(r, way).start()

                        @pl.loop(0, reps - 1)
                        def _(p):
                            sum_share(r, p).start()

            for r, here, onward, way in sides(h):
                @pl.when(here)
                def _():
                    add_dot(r, rep, k)

        if lagged:
            h, k = 1 + lax.div(t - 1, pieces), lax.rem(t - 1, pieces)
            for r, here, onward, way in sides(h):
                @pl.when(here)
                def _():
                    peers_done(r, k)

    steps = (n - 1) * pieces
    step(jnp.int32(0), True, False)

    @pl.loop(1, steps)
    def _(t):
        step(t, True, True)

    step(jnp.int32(steps), False, True)

    @pl.loop(0, n)
    def _(r):
        own = block(r, rep)

        @pl.loop(0, reps - 1)
        def _(p):
            b = r * reps + peer_of(p)
            pltpu.make_async_copy(sums.at[b], sums.at[b], sum_peer.at[p, r]).wait()
            sum_share(r, p).wait_send()
            pltpu.make_async_copy(own, own, pass_sem.at[p, r]).wait()

        for onward, way in (((r >= me) & has_left, 0), ((r <= me) & has_right, 1)):
            @pl.when(onward)
            def _():
                sum_line(r, way).wait_send()
                pltpu.make_async_copy(own, own, send_sem.at[way, r]).wait()

    for s in range(len(bits)):
        trade(s).wait_send()

    if not early:
        tile = 512

        @pl.loop(0, tokens.shape[1] // tile)
        def _(i):
            span = pl.ds(pl.multiple_of(i * tile, tile), tile)
            acc[...] += jnp.dot(
                tokens[:, span], full[span, :], preferred_element_type=jnp.float32
            )

    keys[...] = acc[...].astype(keys.dtype)


def store_kernel(full, keys, sums, weight, probe_keys, checksum, sems):
    parts = 8
    size = full.shape[0] // parts
    copies = [
        pltpu.make_async_copy(
            full.at[pl.ds(i * size, size)], weight.at[pl.ds(i * size, size)], sems.at[i]
        )
        for i in range(parts)
    ]
    copies.append(pltpu.make_async_copy(keys, probe_keys, sems.at[parts]))
    copies.append(pltpu.make_async_copy(sums, checksum, sems.at[parts + 1]))
    for copy in copies:
        copy.start()
    for copy in copies:
        copy.wait()


def body(mesh, master, key_bias, probe_tokens):
    n, reps, heads = mesh.shape["role"], mesh.shape["dp"], mesh.shape["tp"]
    feats, rows = master.shape
    probes, width = probe_tokens.shape
    chunk = min(128, rows)
    pieces, blocks = rows // chunk, n * reps
    levels = heads.bit_length() - 1
    vmem, hbm = pl.BlockSpec(memory_space=pltpu.VMEM), pl.BlockSpec(memory_space=pl.ANY)
    dma = pltpu.SemaphoreType.DMA
    others = max(reps - 1, 1)
    full, keys, sums = pl.pallas_call(
        functools.partial(gather_kernel, n, reps, heads, rows, chunk),
        out_shape=(
            pltpu.VMEM((width, feats), jnp.bfloat16),
            pltpu.VMEM((probes, feats), jnp.bfloat16),
            pltpu.VMEM((blocks, pieces, chunk), jnp.float32),
        ),
        in_specs=[hbm, hbm, hbm],
        out_specs=(vmem, vmem, vmem),
        scratch_shapes=[
            pltpu.VMEM((feats, rows), jnp.float32),
            pltpu.VMEM((probes, width), jnp.bfloat16),
            pltpu.VMEM((1, feats), jnp.float32),
            pltpu.VMEM((probes, feats), jnp.float32),
            pltpu.VMEM((levels, pieces, chunk), jnp.float32),
            pltpu.VMEM((levels, pieces, chunk), jnp.float32),
            dma((min(pieces, 2),)),
            dma,
            dma,
            dma((2, n)),
            dma((n - 1, pieces)),
            dma((others, n)),
            dma((others, n, pieces)),
            dma((levels,)),
            dma((levels,)),
            dma((2, n)),
            dma((n - 1,)),
            dma((others, n)),
            dma((others, n)),
        ],
        compiler_params=pltpu.CompilerParams(
            collective_id=0, has_side_effects=True, vmem_limit_bytes=24 * 2**20
        ),
        name="gather",
    )(
        pltpu.with_memory_space_constraint(master, pltpu.HBM),
        pltpu.with_memory_space_constraint(key_bias.reshape(1, feats), pltpu.HBM),
        pltpu.with_memory_space_constraint(probe_tokens, pltpu.HBM),
    )
    weight, probe_keys, checksum = pl.pallas_call(
        store_kernel,
        out_shape=(
            jax.ShapeDtypeStruct(full.shape, full.dtype),
            jax.ShapeDtypeStruct(keys.shape, keys.dtype),
            jax.ShapeDtypeStruct(sums.shape, sums.dtype),
        ),
        in_specs=[vmem] * 3,
        out_specs=(hbm,) * 3,
        scratch_shapes=[dma((10,))],
        compiler_params=pltpu.CompilerParams(vmem_limit_bytes=2**20),
        name="store",
    )(*(pltpu.with_memory_space_constraint(x, pltpu.VMEM) for x in (full, keys, sums)))
    return weight, probe_keys, checksum.reshape(-1)


def solution(mesh):
    placed = (P("tp", ("role", "dp")), P("tp"), P(("role", "dp"), None))
    return jax.shard_map(
        functools.partial(body, mesh),
        mesh=mesh,
        in_specs=placed,
        out_specs=(P(None, "tp"), P(("role", "dp"), "tp"), P()),
        check_vma=False,
    )
```

```python
import functools

import jax
import jax.numpy as jnp
from jax import lax
from jax.experimental import pallas as pl
from jax.experimental.pallas import tpu as pltpu
from jax.sharding import PartitionSpec as P

MESH = pl.DeviceIdType.MESH


def gather_kernel(
    n, reps, heads, rows, chunk,
    master, bias, probe, full, keys, sums,
    slab, tokens, offset, acc, part, got,
    slab_sem, token_sem, bias_sem, send_sem, line_sem, pass_sem, peer_sem,
    part_send, part_recv, sum_send, sum_recv, sum_pass, sum_peer,
):
    pieces = rows // chunk
    pair = 2 if pieces % 2 == 0 else 1
    span = pair * chunk
    me, rep, head = lax.axis_index("role"), lax.axis_index("dp"), lax.axis_index("tp")
    has_left, has_right = me > 0, me < n - 1
    bits = [1 << s for s in range(heads.bit_length() - 1)]

    def partner(bit):
        return head + bit * (1 - 2 * lax.rem(lax.div(head, bit), 2))

    def peer_of(p):
        return lax.rem(rep + 1 + p, reps)

    barrier = pltpu.get_barrier_semaphore()

    @pl.when(has_left)
    def _():
        pl.semaphore_signal(barrier, inc=1, device_id={"role": me - 1}, device_id_type=MESH)

    @pl.when(has_right)
    def _():
        pl.semaphore_signal(barrier, inc=1, device_id={"role": me + 1}, device_id_type=MESH)

    @pl.loop(0, reps - 1)
    def _(p):
        pl.semaphore_signal(barrier, inc=1, device_id={"dp": peer_of(p)}, device_id_type=MESH)

    for bit in bits:
        pl.semaphore_signal(barrier, inc=1, device_id={"tp": partner(bit)}, device_id_type=MESH)

    cuts = sorted({0, chunk, min(2, pieces) * chunk, rows})

    def slab_copy(i):
        cols = pl.ds(cuts[i], cuts[i + 1] - cuts[i])
        return pltpu.make_async_copy(master.at[:, cols], slab.at[:, cols], slab_sem.at[i])

    slabs = len(cuts) - 1
    token_copy = pltpu.make_async_copy(probe, tokens, token_sem)
    bias_copy = pltpu.make_async_copy(bias, offset, bias_sem)
    for i in range(slabs):
        slab_copy(i).start()
    bias_copy.start()
    token_copy.start()

    def slot(r, owner):
        return lax.rem(r - owner + 2 * n - 1, n)

    def at(r, d, k):
        start = (r * reps + d) * rows + k * chunk
        return full.at[pl.ds(pl.multiple_of(start, chunk), chunk)]

    def group(r, d, g):
        start = (r * reps + d) * rows + g * span
        return full.at[pl.ds(pl.multiple_of(start, span), span)]

    def line(r, k, way):
        return pltpu.make_async_remote_copy(
            src_ref=at(r, rep, k), dst_ref=at(r, rep, k),
            send_sem=send_sem.at[way],
            recv_sem=line_sem.at[slot(r, me + 2 * way - 1), k],
            device_id={"role": me + 2 * way - 1}, device_id_type=MESH,
        )

    def share(r, g, p):
        return pltpu.make_async_remote_copy(
            src_ref=group(r, rep, g), dst_ref=group(r, rep, g),
            send_sem=pass_sem.at[p], recv_sem=peer_sem.at[reps - 2 - p, r, g],
            device_id={"dp": peer_of(p)}, device_id_type=MESH,
        )

    def wait_line(r, k):
        pltpu.make_async_copy(at(r, rep, k), at(r, rep, k), line_sem.at[slot(r, me), k]).wait()

    def wait_peer(r, p, g):
        here = group(r, peer_of(p), g)
        pltpu.make_async_copy(here, here, peer_sem.at[p, r, g]).wait()

    def sum_line(r, way):
        b = r * reps + rep
        return pltpu.make_async_remote_copy(
            src_ref=sums.at[b], dst_ref=sums.at[b],
            send_sem=sum_send.at[way],
            recv_sem=sum_recv.at[slot(r, me + 2 * way - 1)],
            device_id={"role": me + 2 * way - 1}, device_id_type=MESH,
        )

    def sum_share(r, p):
        b = r * reps + rep
        return pltpu.make_async_remote_copy(
            src_ref=sums.at[b], dst_ref=sums.at[b],
            send_sem=sum_pass.at[p], recv_sem=sum_peer.at[reps - 2 - p],
            device_id={"dp": peer_of(p)}, device_id_type=MESH,
        )

    def send_own(k):
        @pl.when(has_left)
        def _():
            line(me, k, 0).start()

        @pl.when(has_right)
        def _():
            line(me, k, 1).start()

        if k % pair == pair - 1:
            @pl.loop(0, reps - 1)
            def _(p):
                share(me, k // pair, p).start()

    for k in range(pieces):
        if k < slabs:
            slab_copy(k).wait()
        held = slab[:, k * chunk : (k + 1) * chunk].astype(jnp.bfloat16).astype(jnp.float32)
        at(me, rep, k)[...] = jnp.transpose(held).astype(jnp.bfloat16)
        part[0, k : k + 1, :] = jnp.sum(held, axis=0, keepdims=True)
        if k == min(1, pieces - 1):
            beside = jnp.where(has_left & has_right, 2, 1) if n > 2 else n - 1
            pl.semaphore_wait(barrier, reps - 1 + len(bits) + beside)
        if k:
            send_own(k - 1)
    bias_copy.wait()
    acc[...] = jnp.broadcast_to(offset[...], acc.shape)
    send_own(pieces - 1)

    def trade(s):
        return pltpu.make_async_remote_copy(
            src_ref=part.at[s], dst_ref=got.at[s],
            send_sem=part_send.at[s], recv_sem=part_recv.at[s],
            device_id={"tp": partner(bits[s])}, device_id_type=MESH,
        )

    early = chunk % 128 == 0

    def add_dot(r, d, g):
        if early:
            start = (r * reps + d) * rows + g * span
            cols = pl.ds(pl.multiple_of(start, span), span)
            acc[...] += jnp.dot(
                tokens[:, cols], group(r, d, g)[...], preferred_element_type=jnp.float32
            )

    def peers_done(r, g):
        @pl.loop(0, reps - 1)
        def _(p):
            wait_peer(r, p, g)
            add_dot(r, peer_of(p), g)

    groups = pieces // pair
    trade(0).start()
    token_copy.wait()

    @pl.loop(0, groups)
    def _(g):
        add_dot(me, rep, g)

    for s in range(len(bits)):
        trade(s).wait_recv()
        total = part[s] + got[s]
        if s + 1 < len(bits):
            part[s + 1] = total
        else:
            sums[me * reps + rep] = total

        @pl.loop(groups * s // len(bits), groups * (s + 1) // len(bits))
        def _(g):
            peers_done(me, g)

        if s + 1 < len(bits):
            trade(s + 1).start()

    @pl.when(has_left)
    def _():
        sum_line(me, 0).start()

    @pl.when(has_right)
    def _():
        sum_line(me, 1).start()

    @pl.loop(0, reps - 1)
    def _(p):
        sum_share(me, p).start()

    def sides(h):
        low, high = me - h, me + h
        return (
            (low, low >= 0, has_right, 1),
            (high, high < n, has_left, 0),
        )

    def step(t, fresh, lagged):
        if fresh:
            h, k = 1 + lax.div(t, pieces), lax.rem(t, pieces)
            g, whole = lax.div(k, pair), lax.rem(k, pair) == pair - 1
            for r, here, onward, way in sides(h):
                @pl.when(here)
                def _():
                    wait_line(r, k)

                    @pl.when(onward)
                    def _():
                        line(r, k, way).start()

                    @pl.when(whole)
                    def _():
                        @pl.loop(0, reps - 1)
                        def _(p):
                            share(r, g, p).start()

                    @pl.when(k == pieces - 1)
                    def _():
                        b = r * reps + rep
                        pltpu.make_async_copy(sums.at[b], sums.at[b], sum_recv.at[slot(r, me)]).wait()

                        @pl.when(onward)
                        def _():
                            sum_line(r, way).start()

                        @pl.loop(0, reps - 1)
                        def _(p):
                            sum_share(r, p).start()

            for r, here, onward, way in sides(h):
                @pl.when(here & whole)
                def _():
                    add_dot(r, rep, g)

        if lagged:
            h, k = 1 + lax.div(t - 1, pieces), lax.rem(t - 1, pieces)
            g, whole = lax.div(k, pair), lax.rem(k, pair) == pair - 1
            for r, here, onward, way in sides(h):
                @pl.when(here & whole)
                def _():
                    peers_done(r, g)

    steps = (n - 1) * pieces
    step(jnp.int32(0), True, False)

    @pl.loop(1, steps)
    def _(t):
        step(t, True, True)

    def drain(ref, sem):
        pltpu.make_async_copy(ref, ref, sem).wait()

    for i in range(n):
        @pl.when(me == i)
        def _():
            for way, count in ((0, n - i if i else 0), (1, i + 1 if i < n - 1 else 0)):
                if count:
                    drain(full.at[pl.ds(0, count * rows)], send_sem.at[way])
                    drain(sums.at[pl.ds(0, count)], sum_send.at[way])

    step(jnp.int32(steps), False, True)

    @pl.loop(0, reps - 1)
    def _(p):
        drain(full.at[pl.ds(0, n * rows)], pass_sem.at[p])
        drain(sums.at[pl.ds(0, n)], sum_pass.at[p])
        drain(sums.at[pl.ds(0, n)], sum_peer.at[p])

    for s in range(len(bits)):
        trade(s).wait_send()

    if not early:
        tile = 512

        @pl.loop(0, tokens.shape[1] // tile)
        def _(i):
            part_of = pl.ds(pl.multiple_of(i * tile, tile), tile)
            acc[...] += jnp.dot(
                tokens[:, part_of], full[part_of, :], preferred_element_type=jnp.float32
            )

    keys[...] = acc[...].astype(keys.dtype)


def store_kernel(full, keys, sums, weight, probe_keys, checksum, sems):
    parts = 8
    size = full.shape[0] // parts
    copies = [
        pltpu.make_async_copy(
            full.at[pl.ds(i * size, size)], weight.at[pl.ds(i * size, size)], sems.at[i]
        )
        for i in range(parts)
    ]
    copies.append(pltpu.make_async_copy(keys, probe_keys, sems.at[parts]))
    copies.append(pltpu.make_async_copy(sums, checksum, sems.at[parts + 1]))
    for copy in copies:
        copy.start()
    for copy in copies:
        copy.wait()


def body(mesh, master, key_bias, probe_tokens):
    n, reps, heads = mesh.shape["role"], mesh.shape["dp"], mesh.shape["tp"]
    feats, rows = master.shape
    probes, width = probe_tokens.shape
    chunk = min(128, rows)
    pieces, blocks = rows // chunk, n * reps
    levels = heads.bit_length() - 1
    groups = pieces // 2 if pieces % 2 == 0 else pieces
    vmem, hbm = pl.BlockSpec(memory_space=pltpu.VMEM), pl.BlockSpec(memory_space=pl.ANY)
    dma = pltpu.SemaphoreType.DMA
    others = max(reps - 1, 1)
    full, keys, sums = pl.pallas_call(
        functools.partial(gather_kernel, n, reps, heads, rows, chunk),
        out_shape=(
            pltpu.VMEM((width, feats), jnp.bfloat16),
            pltpu.VMEM((probes, feats), jnp.bfloat16),
            pltpu.VMEM((blocks, pieces, chunk), jnp.float32),
        ),
        in_specs=[hbm, hbm, hbm],
        out_specs=(vmem, vmem, vmem),
        scratch_shapes=[
            pltpu.VMEM((feats, rows), jnp.float32),
            pltpu.VMEM((probes, width), jnp.bfloat16),
            pltpu.VMEM((1, feats), jnp.float32),
            pltpu.VMEM((probes, feats), jnp.float32),
            pltpu.VMEM((levels, pieces, chunk), jnp.float32),
            pltpu.VMEM((levels, pieces, chunk), jnp.float32),
            dma((min(pieces, 3),)),
            dma,
            dma,
            dma((2,)),
            dma((n - 1, pieces)),
            dma((others,)),
            dma((others, n, groups)),
            dma((levels,)),
            dma((levels,)),
            dma((2,)),
            dma((n - 1,)),
            dma((others,)),
            dma((others,)),
        ],
        compiler_params=pltpu.CompilerParams(
            collective_id=0, has_side_effects=True, vmem_limit_bytes=24 * 2**20
        ),
        name="gather",
    )(
        pltpu.with_memory_space_constraint(master, pltpu.HBM),
        pltpu.with_memory_space_constraint(key_bias.reshape(1, feats), pltpu.HBM),
        pltpu.with_memory_space_constraint(probe_tokens, pltpu.HBM),
    )
    weight, probe_keys, checksum = pl.pallas_call(
        store_kernel,
        out_shape=(
            jax.ShapeDtypeStruct(full.shape, full.dtype),
            jax.ShapeDtypeStruct(keys.shape, keys.dtype),
            jax.ShapeDtypeStruct(sums.shape, sums.dtype),
        ),
        in_specs=[vmem] * 3,
        out_specs=(hbm,) * 3,
        scratch_shapes=[dma((10,))],
        compiler_params=pltpu.CompilerParams(vmem_limit_bytes=2**20),
        name="store",
    )(*(pltpu.with_memory_space_constraint(x, pltpu.VMEM) for x in (full, keys, sums)))
    return weight, probe_keys, checksum.reshape(-1)


def solution(mesh):
    placed = (P("tp", ("role", "dp")), P("tp"), P(("role", "dp"), None))
    return jax.shard_map(
        functools.partial(body, mesh),
        mesh=mesh,
        in_specs=placed,
        out_specs=(P(None, "tp"), P(("role", "dp"), "tp"), P()),
        check_vma=False,
    )
```

```python
import functools

import jax
import jax.numpy as jnp
from jax import lax
from jax.experimental import pallas as pl
from jax.experimental.pallas import tpu as pltpu
from jax.sharding import PartitionSpec as P

MESH = pl.DeviceIdType.MESH


def gather_kernel(
    n, reps, heads, rows, chunk,
    master, bias, probe, full, keys, sums,
    slab, tokens, offset, acc, part, got,
    slab_sem, token_sem, bias_sem, send_sem, line_sem, pass_sem, peer_sem,
    part_send, part_recv, sum_send, sum_recv, sum_pass, sum_peer,
):
    pieces = rows // chunk
    pair = 2 if pieces % 2 == 0 else 1
    span = pair * chunk
    me, rep, head = lax.axis_index("role"), lax.axis_index("dp"), lax.axis_index("tp")
    has_left, has_right = me > 0, me < n - 1
    bits = [1 << s for s in range(heads.bit_length() - 1)]

    def partner(bit):
        return head + bit * (1 - 2 * lax.rem(lax.div(head, bit), 2))

    def peer_of(p):
        return lax.rem(rep + 1 + p, reps)

    cuts = sorted({0, chunk, min(2, pieces) * chunk, rows})

    def slab_copy(i):
        cols = pl.ds(cuts[i], cuts[i + 1] - cuts[i])
        return pltpu.make_async_copy(master.at[:, cols], slab.at[:, cols], slab_sem.at[i])

    slabs = len(cuts) - 1
    for i in range(slabs):
        slab_copy(i).start()

    barrier = pltpu.get_barrier_semaphore()

    @pl.when(has_left)
    def _():
        pl.semaphore_signal(barrier, inc=1, device_id={"role": me - 1}, device_id_type=MESH)

    @pl.when(has_right)
    def _():
        pl.semaphore_signal(barrier, inc=1, device_id={"role": me + 1}, device_id_type=MESH)

    @pl.loop(0, reps - 1)
    def _(p):
        pl.semaphore_signal(barrier, inc=1, device_id={"dp": peer_of(p)}, device_id_type=MESH)

    for bit in bits:
        pl.semaphore_signal(barrier, inc=1, device_id={"tp": partner(bit)}, device_id_type=MESH)

    token_copy = pltpu.make_async_copy(probe, tokens, token_sem)
    bias_copy = pltpu.make_async_copy(bias, offset, bias_sem)
    bias_copy.start()
    token_copy.start()

    def slot(r, owner):
        return lax.rem(r - owner + 2 * n - 1, n)

    def at(r, d, k):
        start = (r * reps + d) * rows + k * chunk
        return full.at[pl.ds(pl.multiple_of(start, chunk), chunk)]

    def group(r, d, g):
        start = (r * reps + d) * rows + g * span
        return full.at[pl.ds(pl.multiple_of(start, span), span)]

    def line(r, k, way):
        return pltpu.make_async_remote_copy(
            src_ref=at(r, rep, k), dst_ref=at(r, rep, k),
            send_sem=send_sem.at[way],
            recv_sem=line_sem.at[slot(r, me + 2 * way - 1), k],
            device_id={"role": me + 2 * way - 1}, device_id_type=MESH,
        )

    def share(r, k, p):
        return pltpu.make_async_remote_copy(
            src_ref=at(r, rep, k), dst_ref=at(r, rep, k),
            send_sem=pass_sem.at[p],
            recv_sem=peer_sem.at[reps - 2 - p, r, lax.div(k, pair)],
            device_id={"dp": peer_of(p)}, device_id_type=MESH,
        )

    def wait_line(r, k):
        pltpu.make_async_copy(at(r, rep, k), at(r, rep, k), line_sem.at[slot(r, me), k]).wait()

    def wait_peer(r, p, g):
        here = group(r, peer_of(p), g)
        pltpu.make_async_copy(here, here, peer_sem.at[p, r, g]).wait()

    def sum_line(r, way):
        b = r * reps + rep
        return pltpu.make_async_remote_copy(
            src_ref=sums.at[b], dst_ref=sums.at[b],
            send_sem=sum_send.at[way],
            recv_sem=sum_recv.at[slot(r, me + 2 * way - 1)],
            device_id={"role": me + 2 * way - 1}, device_id_type=MESH,
        )

    def sum_share(r, p):
        b = r * reps + rep
        return pltpu.make_async_remote_copy(
            src_ref=sums.at[b], dst_ref=sums.at[b],
            send_sem=sum_pass.at[p], recv_sem=sum_peer.at[reps - 2 - p],
            device_id={"dp": peer_of(p)}, device_id_type=MESH,
        )

    def send_own(k):
        @pl.when(has_left)
        def _():
            line(me, k, 0).start()

        @pl.when(has_right)
        def _():
            line(me, k, 1).start()

        @pl.loop(0, reps - 1)
        def _(p):
            share(me, jnp.int32(k), p).start()

    for k in range(pieces):
        if k < slabs:
            slab_copy(k).wait()
        held = slab[:, k * chunk : (k + 1) * chunk].astype(jnp.bfloat16).astype(jnp.float32)
        at(me, rep, k)[...] = jnp.transpose(held).astype(jnp.bfloat16)
        part[0, k : k + 1, :] = jnp.sum(held, axis=0, keepdims=True)
        if k == min(1, pieces - 1):
            beside = jnp.where(has_left & has_right, 2, 1) if n > 2 else n - 1
            pl.semaphore_wait(barrier, reps - 1 + len(bits) + beside)
        if k:
            send_own(k - 1)
    bias_copy.wait()
    acc[...] = jnp.broadcast_to(offset[...], acc.shape)
    send_own(pieces - 1)

    def trade(s):
        return pltpu.make_async_remote_copy(
            src_ref=part.at[s], dst_ref=got.at[s],
            send_sem=part_send.at[s], recv_sem=part_recv.at[s],
            device_id={"tp": partner(bits[s])}, device_id_type=MESH,
        )

    early = chunk % 128 == 0

    def add_dot(r, d, g):
        if early:
            start = (r * reps + d) * rows + g * span
            cols = pl.ds(pl.multiple_of(start, span), span)
            acc[...] += jnp.dot(
                tokens[:, cols], group(r, d, g)[...], preferred_element_type=jnp.float32
            )

    def peers_done(r, g):
        @pl.loop(0, reps - 1)
        def _(p):
            wait_peer(r, p, g)
            add_dot(r, peer_of(p), g)

    groups = pieces // pair
    trade(0).start()
    token_copy.wait()

    @pl.loop(0, groups)
    def _(g):
        add_dot(me, rep, g)

    for s in range(len(bits)):
        trade(s).wait_recv()
        total = part[s] + got[s]
        if s + 1 < len(bits):
            part[s + 1] = total
        else:
            sums[me * reps + rep] = total

        @pl.loop(groups * s // len(bits), groups * (s + 1) // len(bits))
        def _(g):
            peers_done(me, g)

        if s + 1 < len(bits):
            trade(s + 1).start()

    @pl.when(has_left)
    def _():
        sum_line(me, 0).start()

    @pl.when(has_right)
    def _():
        sum_line(me, 1).start()

    @pl.loop(0, reps - 1)
    def _(p):
        sum_share(me, p).start()

    def sides(h):
        low, high = me - h, me + h
        return (
            (low, low >= 0, has_right, 1),
            (high, high < n, has_left, 0),
        )

    def step(t, fresh, lagged):
        if fresh:
            h, k = 1 + lax.div(t, pieces), lax.rem(t, pieces)
            g, whole = lax.div(k, pair), lax.rem(k, pair) == pair - 1
            for r, here, onward, way in sides(h):
                @pl.when(here)
                def _():
                    wait_line(r, k)

                    @pl.when(onward)
                    def _():
                        line(r, k, way).start()

                    @pl.loop(0, reps - 1)
                    def _(p):
                        share(r, k, p).start()

                    @pl.when(k == pieces - 1)
                    def _():
                        b = r * reps + rep
                        pltpu.make_async_copy(sums.at[b], sums.at[b], sum_recv.at[slot(r, me)]).wait()

                        @pl.when(onward)
                        def _():
                            sum_line(r, way).start()

                        @pl.loop(0, reps - 1)
                        def _(p):
                            sum_share(r, p).start()

            for r, here, onward, way in sides(h):
                @pl.when(here & whole)
                def _():
                    add_dot(r, rep, g)

        if lagged:
            h, k = 1 + lax.div(t - 1, pieces), lax.rem(t - 1, pieces)
            g, whole = lax.div(k, pair), lax.rem(k, pair) == pair - 1
            for r, here, onward, way in sides(h):
                @pl.when(here & whole)
                def _():
                    peers_done(r, g)

    steps = (n - 1) * pieces
    step(jnp.int32(0), True, False)

    @pl.loop(1, steps)
    def _(t):
        step(t, True, True)

    def drain(ref, sem):
        pltpu.make_async_copy(ref, ref, sem).wait()

    for i in range(n):
        @pl.when(me == i)
        def _():
            for way, count in ((0, n - i if i else 0), (1, i + 1 if i < n - 1 else 0)):
                if count:
                    drain(full.at[pl.ds(0, count * rows)], send_sem.at[way])
                    drain(sums.at[pl.ds(0, count)], sum_send.at[way])

    step(jnp.int32(steps), False, True)

    @pl.loop(0, reps - 1)
    def _(p):
        drain(full.at[pl.ds(0, n * rows)], pass_sem.at[p])
        drain(sums.at[pl.ds(0, n)], sum_pass.at[p])
        drain(sums.at[pl.ds(0, n)], sum_peer.at[p])

    for s in range(len(bits)):
        trade(s).wait_send()

    if not early:
        tile = 512

        @pl.loop(0, tokens.shape[1] // tile)
        def _(i):
            part_of = pl.ds(pl.multiple_of(i * tile, tile), tile)
            acc[...] += jnp.dot(
                tokens[:, part_of], full[part_of, :], preferred_element_type=jnp.float32
            )

    keys[...] = acc[...].astype(keys.dtype)


def store_kernel(full, keys, sums, weight, probe_keys, checksum, sems):
    parts = 8
    size = full.shape[0] // parts
    copies = [
        pltpu.make_async_copy(
            full.at[pl.ds(i * size, size)], weight.at[pl.ds(i * size, size)], sems.at[i]
        )
        for i in range(parts)
    ]
    copies.append(pltpu.make_async_copy(keys, probe_keys, sems.at[parts]))
    copies.append(pltpu.make_async_copy(sums, checksum, sems.at[parts + 1]))
    for copy in copies:
        copy.start()
    for copy in copies:
        copy.wait()


def body(mesh, master, key_bias, probe_tokens):
    n, reps, heads = mesh.shape["role"], mesh.shape["dp"], mesh.shape["tp"]
    feats, rows = master.shape
    probes, width = probe_tokens.shape
    chunk = min(128, rows)
    pieces, blocks = rows // chunk, n * reps
    levels = heads.bit_length() - 1
    groups = pieces // 2 if pieces % 2 == 0 else pieces
    vmem, hbm = pl.BlockSpec(memory_space=pltpu.VMEM), pl.BlockSpec(memory_space=pl.ANY)
    dma = pltpu.SemaphoreType.DMA
    others = max(reps - 1, 1)
    full, keys, sums = pl.pallas_call(
        functools.partial(gather_kernel, n, reps, heads, rows, chunk),
        out_shape=(
            pltpu.VMEM((width, feats), jnp.bfloat16),
            pltpu.VMEM((probes, feats), jnp.bfloat16),
            pltpu.VMEM((blocks, pieces, chunk), jnp.float32),
        ),
        in_specs=[hbm, hbm, hbm],
        out_specs=(vmem, vmem, vmem),
        scratch_shapes=[
            pltpu.VMEM((feats, rows), jnp.float32),
            pltpu.VMEM((probes, width), jnp.bfloat16),
            pltpu.VMEM((1, feats), jnp.float32),
            pltpu.VMEM((probes, feats), jnp.float32),
            pltpu.VMEM((levels, pieces, chunk), jnp.float32),
            pltpu.VMEM((levels, pieces, chunk), jnp.float32),
            dma((min(pieces, 3),)),
            dma,
            dma,
            dma((2,)),
            dma((n - 1, pieces)),
            dma((others,)),
            dma((others, n, groups)),
            dma((levels,)),
            dma((levels,)),
            dma((2,)),
            dma((n - 1,)),
            dma((others,)),
            dma((others,)),
        ],
        compiler_params=pltpu.CompilerParams(
            collective_id=0, has_side_effects=True, vmem_limit_bytes=24 * 2**20
        ),
        name="gather",
    )(
        pltpu.with_memory_space_constraint(master, pltpu.HBM),
        pltpu.with_memory_space_constraint(key_bias.reshape(1, feats), pltpu.HBM),
        pltpu.with_memory_space_constraint(probe_tokens, pltpu.HBM),
    )
    weight, probe_keys, checksum = pl.pallas_call(
        store_kernel,
        out_shape=(
            jax.ShapeDtypeStruct(full.shape, full.dtype),
            jax.ShapeDtypeStruct(keys.shape, keys.dtype),
            jax.ShapeDtypeStruct(sums.shape, sums.dtype),
        ),
        in_specs=[vmem] * 3,
        out_specs=(hbm,) * 3,
        scratch_shapes=[dma((10,))],
        compiler_params=pltpu.CompilerParams(vmem_limit_bytes=2**20),
        name="store",
    )(*(pltpu.with_memory_space_constraint(x, pltpu.VMEM) for x in (full, keys, sums)))
    return weight, probe_keys, checksum.reshape(-1)


def solution(mesh):
    placed = (P("tp", ("role", "dp")), P("tp"), P(("role", "dp"), None))
    return jax.shard_map(
        functools.partial(body, mesh),
        mesh=mesh,
        in_specs=placed,
        out_specs=(P(None, "tp"), P(("role", "dp"), "tp"), P()),
        check_vma=False,
    )
```
